256 devices in a mesh: ka: 32 (over z_hi, x, y), ga: 8 (over z_lo, core).
Axes of the slice: x: 4, y: 4, z: 8 (z_hi: 2, z_lo: 4; z = z_hi * 4 + z_lo), core: 2. Of those that a mesh axis runs over, the one named last changes fastest.
Arguments:
- psi: bfloat16 [32, 2, 128, 2048], P('ka', None, None, 'ga'), may hold values from -0.62890625 to 0.62890625
- dvscf: bfloat16 [96, 2, 2048], P(None, None, 'ga'), may hold values from -6 to 6
- kq_map: int32 [32], P('ka'), may hold values from 0 to 31, each once
Outputs:
- coupling: float32 [96, 32, 2, 128, 128], P('ga', 'ka')
The draws below stay inside these ranges and needn't reach their ends.
Inputs may be any that keep to these rules, and one draw needn't show every extreme that they name: kq_map is a permutation of the k-points 0 to 31.
All inputs are finite; a program needn't handle non-finite values.
Results may differ from the reference program's by a relative error of at most 0.0029.
Values may be sent and summed in bfloat16 or wider, within the bound.
No kernel may reach another device: no remote copies, remote signals or barrier semaphores. Data moves between devices by JAX's collectives and lax.ppermute only.
A program may use at most 128 MiB of HBM per device.

```python
import jax
import jax.numpy as jnp
from jax import lax

BANDS = 128
MODES = 96
KPTS = 32
CELLS = 2048


def block_scale(stream_key, shape, cuts, least, high):
    loudness = 1.0
    for dim, parts in cuts:
        steps = jax.random.uniform(jax.random.fold_in(jax.random.fold_in(stream_key, 6), dim), (parts,), jnp.float32, least / len(cuts), high / len(cuts))
        loudness = loudness * jnp.repeat(jnp.exp(steps), shape[dim] // parts).reshape((-1,) + (1,) * (len(shape) - 1 - dim))
    return loudness


def noise(stream_key, shape, width, reach, cuts=(), dtype=jnp.bfloat16):
    values = width * jax.random.normal(stream_key, shape, jnp.float32)
    if cuts:
        values = values * block_scale(stream_key, shape, cuts, -0.22, 0.18)
    return jnp.clip(values, -reach, reach).astype(dtype)


def setup_inputs(seed: int = 0) -> dict:
    key_list = jax.random.split(jax.random.key(seed), 4)
    return {
        "psi": noise(key_list[0], (KPTS, 2, BANDS, CELLS), ((4 * CELLS) ** -0.25), 0.62890625, ((0, 32), (3, 8))),
        "dvscf": noise(key_list[1], (MODES, 2, CELLS), 1.0, 6.0, ((2, 8),)),
        "kq_map": jax.random.permutation(key_list[2], KPTS).astype(jnp.int32),
    }


def reference(psi, dvscf, kq_map):
    phi_all = jnp.take(psi, kq_map.astype(jnp.int32), axis=0)
    dv_real = dvscf[:, 0].astype(jnp.float32)[:, None, :]
    dv_imag = dvscf[:, 1].astype(jnp.float32)[:, None, :]

    def per_point(pair):
        wave, other = pair
        wave_real = wave[0].astype(jnp.float32)[None]
        wave_imag = wave[1].astype(jnp.float32)[None]
        prod_real = (dv_real * wave_real - dv_imag * wave_imag).astype(jnp.bfloat16)
        prod_imag = (dv_real * wave_imag + dv_imag * wave_real).astype(jnp.bfloat16)
        left = jnp.concatenate([other[0], other[1]], axis=-1).astype(jnp.float32)
        right_real = jnp.concatenate([prod_real, prod_imag], axis=-1).astype(jnp.float32)
        right_imag = jnp.concatenate([prod_imag, -prod_real], axis=-1).astype(jnp.float32)
        part_real = jnp.einsum('mr,unr->umn', left, right_real)
        part_imag = jnp.einsum('mr,unr->umn', left, right_imag)
        return jnp.stack([part_real, part_imag], axis=1)

    result = lax.map(per_point, (psi, phi_all))
    return jnp.transpose(result, (1, 0, 2, 3, 4))
```

```python
import jax
import jax.numpy as jnp
from jax import lax
from jax.experimental import pallas as pl
from jax.experimental.pallas import tpu as pltpu
from jax.sharding import Mesh
from jax.sharding import PartitionSpec as P

KA = ("zh", "x", "y")
GA = ("zl", "c")
SWAP = [(0, 1), (1, 0)]


def ring(step, size=4):
    return [(i, (i + step) % size) for i in range(size)]


def couple(half, waves, others, potentials, modes):
    parts = len(waves)
    bands, cells = waves[0].shape[0] // 2, waves[0].shape[1]
    wide = parts * cells

    def kernel(half_ref, *refs):
        wave_refs, other_refs, pot_refs = refs[:parts], refs[parts : 2 * parts], refs[2 * parts : 3 * parts]
        out_ref = refs[3 * parts]
        wave_re, wave_im, left, right_a, right_b = refs[3 * parts + 1 :]
        step = pl.program_id(0)
        first = half_ref[0] * modes

        def fill(mode, right):
            for p in range(parts):
                at = slice(p * cells, (p + 1) * cells)
                dv_re = pot_refs[p][mode, 0:1, :].astype(jnp.float32)
                dv_im = pot_refs[p][mode, 1:2, :].astype(jnp.float32)
                w_re, w_im = wave_re[:, at], wave_im[:, at]
                right[:bands, at] = (dv_re * w_re - dv_im * w_im).astype(jnp.bfloat16)
                right[bands:, at] = (dv_re * w_im + dv_im * w_re).astype(jnp.bfloat16)

        def finish(slot, right):
            full = lax.dot_general(left[...], right[...], (((1,), (1,)), ((), ())), preferred_element_type=jnp.float32)
            out_ref[slot, 0] = full[:bands, :bands] + full[bands:, bands:]
            out_ref[slot, 1] = full[:bands, bands:] - full[bands:, :bands]

        @pl.when(step == 0)
        def _():
            for p in range(parts):
                at = slice(p * cells, (p + 1) * cells)
                wave_re[:, at] = wave_refs[p][:bands].astype(jnp.float32)
                wave_im[:, at] = wave_refs[p][bands:].astype(jnp.float32)
                left[:, at] = other_refs[p][...]
            fill(first, right_a)

        fill(first + 2 * step + 1, right_b)
        finish(0, right_a)
        fill(first + jnp.minimum(2 * step + 2, modes - 1), right_a)
        finish(1, right_b)

    whole = lambda a: pl.BlockSpec(a.shape, lambda i: (0,) * a.ndim)
    return pl.pallas_call(
        kernel,
        grid=(modes // 2,),
        in_specs=[pl.BlockSpec(memory_space=pltpu.SMEM)] + [whole(a) for a in (*waves, *others, *potentials)],
        out_specs=pl.BlockSpec((2, 2, bands, bands), lambda i: (i, 0, 0, 0)),
        out_shape=jax.ShapeDtypeStruct((modes, 2, bands, bands), jnp.float32),
        scratch_shapes=[
            pltpu.VMEM((bands, wide), jnp.float32),
            pltpu.VMEM((bands, wide), jnp.float32),
            pltpu.VMEM((2 * bands, wide), jnp.bfloat16),
            pltpu.VMEM((2 * bands, wide), jnp.bfloat16),
            pltpu.VMEM((2 * bands, wide), jnp.bfloat16),
        ],
        compiler_params=pltpu.CompilerParams(dimension_semantics=("arbitrary",)),
    )(half, *waves, *others, *potentials)


def pick(number, choices):
    out = choices[0]
    for i, choice in enumerate(choices[1:], 1):
        out = jnp.where(number == i, choice, out)
    return out


def body(psi, dvscf, kq_map):
    zh, x, y, zl, c = (lax.axis_index(a) for a in ("zh", "x", "y", "zl", "c"))
    bands, cells = psi.shape[2], psi.shape[3]
    slab = psi.reshape(2 * bands, cells)
    chip_modes = dvscf.shape[0] // 4
    modes = chip_modes // 2

    swapped = lax.ppermute(slab, "zh", SWAP)
    near = [slab] + [lax.ppermute(slab, "y", ring(s)) for s in (1, 2, 3)]
    wanted = [kq_map] + [lax.ppermute(kq_map, "x", ring(-s)) for s in (1, 2, 3)]
    far = [swapped] + [lax.ppermute(swapped, "y", ring(s)) for s in (1, 2, 3)]
    slots = []
    for k in wanted:
        source = k[0]
        back = (y - source % 4) % 4
        slots.append(pick(jnp.where(source // 16 == zh, back, back + 4), near + far))
    came = [slots[0]] + [lax.ppermute(slots[s], "x", ring(s)) for s in (1, 2, 3)]
    phi = pick((x - (kq_map[0] // 4) % 4) % 4, came)

    slab_late, _ = lax.optimization_barrier((slab, swapped))
    waves = [slab] + [lax.ppermute(slab_late, "zl", ring(s)) for s in (1, 3, 2)]
    potentials = []
    for s in (0, 1, 3, 2):
        part = lax.dynamic_slice_in_dim(dvscf, chip_modes * ((zl + s) % 4), chip_modes, 0)
        potentials.append(lax.ppermute(part, "zl", ring(s)) if s else part)
    others = [phi] + [lax.ppermute(phi, "zl", ring(s)) for s in (1, 3, 2)]

    theirs = couple((1 - c)[None].astype(jnp.int32), waves, others, potentials, modes)
    theirs = lax.ppermute(theirs, "c", SWAP)
    mine = couple(c[None].astype(jnp.int32), waves, others, potentials, modes)
    return (mine + theirs)[:, None]


def solution(mesh):
    finer = Mesh(mesh.devices.reshape(2, 4, 4, 4, 2), KA + GA)
    in_specs = (P(KA, None, None, GA), P(None, None, GA), P(KA))
    out_specs = P(GA, KA, None, None, None)
    return jax.shard_map(body, mesh=finer, in_specs=in_specs, out_specs=out_specs, check_vma=False)
```

```python
import jax
import jax.numpy as jnp
from jax import lax
from jax.experimental import pallas as pl
from jax.experimental.pallas import tpu as pltpu
from jax.sharding import Mesh
from jax.sharding import PartitionSpec as P

KA = ("zh", "x", "y")
GA = ("zl", "c")
SWAP = [(0, 1), (1, 0)]
STEPS = (1, 3, 2)


def ring(step, size=4):
    return [(i, (i + step) % size) for i in range(size)]


def pack(zl, slab, potential):
    rows, cells = slab.shape
    share = potential.shape[0] // 4

    def kernel(zl_ref, slab_ref, pot_ref, *outs):
        for s, out in enumerate(outs):
            out[:rows] = slab_ref[...]
            first = pl.multiple_of(share * lax.rem(zl_ref[0] + s, 4), share)
            out[rows:] = pot_ref[pl.ds(first, share), :]

    return pl.pallas_call(
        kernel,
        in_specs=[pl.BlockSpec(memory_space=pltpu.SMEM), pl.BlockSpec(memory_space=pltpu.VMEM), pl.BlockSpec(memory_space=pltpu.VMEM)],
        out_shape=[jax.ShapeDtypeStruct((rows + share, cells), slab.dtype)] * 4,
    )(zl, slab, potential)


def couple(core, packs, others, bands, modes, per_step):
    parts = len(others)
    cells = others[0].shape[1]
    wide = parts * cells
    rows = 2 * bands
    share = packs[0].shape[-2] - rows
    count = len(packs)

    def kernel(core_ref, *refs):
        pack_refs, other_refs = refs[:count], refs[count : count + parts]
        out_ref = refs[count + parts]
        wave_re, wave_im, pots, left, right_a, right_b = refs[count + parts + 1 :]
        step = pl.program_id(0)
        first = core_ref[0] * (share // 2)
        pieces = []
        for ref in pack_refs:
            if len(ref.shape) == 3:
                pieces += [ref.at[i] for i in range(ref.shape[0])]
            else:
                pieces.append(ref)

        def fill(mode, right):
            for p in range(parts):
                at = slice(p * cells, (p + 1) * cells)
                dv_re = pots[pl.ds(first + 2 * mode, 1), at]
                dv_im = pots[pl.ds(first + 2 * mode + 1, 1), at]
                w_re, w_im = wave_re[:, at], wave_im[:, at]
                right[:bands, at] = (dv_re * w_re - dv_im * w_im).astype(jnp.bfloat16)
                right[bands:, at] = (dv_re * w_im + dv_im * w_re).astype(jnp.bfloat16)

        def finish(slot, right):
            full = lax.dot_general(left[...], right[...], (((1,), (1,)), ((), ())), preferred_element_type=jnp.float32)
            out_ref[slot, 0] = full[:bands, :bands] + full[bands:, bands:]
            out_ref[slot, 1] = full[:bands, bands:] - full[bands:, :bands]

        @pl.when(step == 0)
        def _():
            for p in range(parts):
                at = slice(p * cells, (p + 1) * cells)
                wave_re[:, at] = pieces[p][:bands].astype(jnp.float32)
                wave_im[:, at] = pieces[p][bands:rows].astype(jnp.float32)
                pots[:, at] = pieces[p][rows:].astype(jnp.float32)
                left[:, at] = other_refs[p][...]

        for j in range(0, per_step, 2):
            fill(step * per_step + j, right_a)
            fill(step * per_step + j + 1, right_b)
            finish(j, right_a)
            finish(j + 1, right_b)

    whole = lambda a: pl.BlockSpec(a.shape, lambda i: (0,) * a.ndim)
    return pl.pallas_call(
        kernel,
        grid=(modes // per_step,),
        in_specs=[pl.BlockSpec(memory_space=pltpu.SMEM)] + [whole(a) for a in (*packs, *others)],
        out_specs=pl.BlockSpec((per_step, 2, bands, bands), lambda i: (i, 0, 0, 0)),
        out_shape=jax.ShapeDtypeStruct((modes, 2, bands, bands), jnp.float32),
        scratch_shapes=[
            pltpu.VMEM((bands, wide), jnp.float32),
            pltpu.VMEM((bands, wide), jnp.float32),
            pltpu.VMEM((share, wide), jnp.float32),
            pltpu.VMEM((rows, wide), jnp.bfloat16),
            pltpu.VMEM((rows, wide), jnp.bfloat16),
            pltpu.VMEM((rows, wide), jnp.bfloat16),
        ],
        compiler_params=pltpu.CompilerParams(dimension_semantics=("arbitrary",)),
    )(core, *packs, *others)


def pick(number, choices):
    out = choices[0]
    for i, choice in enumerate(choices[1:], 1):
        out = jnp.where(number == i, choice, out)
    return out


def body(psi, dvscf, kq_map):
    zh, x, y, zl, c = (lax.axis_index(a) for a in ("zh", "x", "y", "zl", "c"))
    bands, cells = psi.shape[2], psi.shape[3]
    modes = dvscf.shape[0] // 8
    slab = psi.reshape(2 * bands, cells)

    swapped = lax.ppermute(slab, "zh", SWAP)
    near = [slab] + [lax.ppermute(slab, "y", ring(s)) for s in (1, 2, 3)]
    far = [swapped] + [lax.ppermute(swapped, "y", ring(s)) for s in (1, 2, 3)]
    wanted = [kq_map] + [lax.ppermute(kq_map, "x", ring(-s)) for s in (1, 2, 3)]

    packs = pack(zl[None], slab, dvscf.reshape(-1, cells))
    lines = [packs[0]] + [lax.ppermute(packs[s], "zl", ring(s)) for s in STEPS]
    lines = jnp.stack(lines)
    twins = lax.ppermute(lines, "c", SWAP)

    slots = []
    for k in wanted:
        source = k[0]
        back = (y - source % 4) % 4
        slots.append(pick(jnp.where(source // 16 == zh, back, back + 4), near + far))
    came = [slots[0]] + [lax.ppermute(slots[s], "x", ring(s)) for s in (1, 2, 3)]
    phi = pick((x - (kq_map[0] // 4) % 4) % 4, came)

    others = [phi] + [lax.ppermute(phi, "zl", ring(s)) for s in STEPS]
    others += [lax.ppermute(o, "c", SWAP) for o in others]
    out = couple(c[None], [lines, twins], others, bands, modes, 4)
    return out[:, None]


def solution(mesh):
    finer = Mesh(mesh.devices.reshape(2, 4, 4, 4, 2), KA + GA)
    in_specs = (P(KA, None, None, GA), P(None, None, GA), P(KA))
    out_specs = P(GA, KA, None, None, None)
    return jax.shard_map(body, mesh=finer, in_specs=in_specs, out_specs=out_specs, check_vma=False)
```

```python
import jax
import jax.numpy as jnp
from jax import lax
from jax.experimental import pallas as pl
from jax.experimental.pallas import tpu as pltpu
from jax.sharding import Mesh
from jax.sharding import PartitionSpec as P

KA = ("zh", "x", "y")
GA = ("zl", "c")
XY = ("x", "y")
SWAP = [(0, 1), (1, 0)]
MIRROR = [(z, 7 - z) for z in range(8)]
STEPS = (0, 1, 3, 2)
TAG = 8
IN_SMEM = pl.BlockSpec(memory_space=pltpu.SMEM)
IN_VMEM = pl.BlockSpec(memory_space=pltpu.VMEM)


def ring(step, size=4):
    return [(i, (i + step) % size) for i in range(size)]


def pack_lines(slab, potential):
    rows, cells = slab.shape
    modes = potential.shape[0] // 4

    def kernel(slab_ref, pot_ref, *outs):
        zl = lax.axis_index("zl")
        for s, out in zip(STEPS, outs):
            out[:rows] = slab_ref[...]
            first = modes * lax.rem(zl + s, 4)
            for m in range(modes):
                out[rows + 2 * m : rows + 2 * m + 2] = pot_ref[first + m]

    return pl.pallas_call(
        kernel,
        in_specs=[IN_VMEM, IN_VMEM],
        out_shape=[jax.ShapeDtypeStruct((rows + 2 * modes, cells), slab.dtype)] * 4,
    )(slab, potential)


def pack_spread(slab, swapped, kq):
    rows, cells = slab.shape
    piece = rows // 16

    def kernel(kq_ref, slab_ref, swapped_ref, out):
        tag = jnp.full((TAG, cells), kq_ref[0].astype(jnp.float32)).astype(slab.dtype)
        for j in range(16):
            out[j, :piece] = slab_ref[j * piece : (j + 1) * piece]
            out[j, piece : 2 * piece] = swapped_ref[j * piece : (j + 1) * piece]
            out[j, 2 * piece :] = tag

    return pl.pallas_call(
        kernel,
        in_specs=[IN_SMEM, IN_VMEM, IN_VMEM],
        out_shape=jax.ShapeDtypeStruct((16, 2 * piece + TAG, cells), slab.dtype),
    )(kq, slab, swapped)


def choose(pieces):
    count, rows, cells = pieces.shape
    piece = (rows - TAG) // 2

    def kernel(ref, out):
        zh = lax.axis_index("zh")
        for d in range(count):
            source = jnp.max(ref[d, 2 * piece :, :128].astype(jnp.float32)).astype(jnp.int32)
            side = jnp.where(source // count == zh, 0, piece)
            out[d] = ref[lax.rem(source, count), pl.ds(pl.multiple_of(side, piece), piece), :]

    return pl.pallas_call(
        kernel,
        in_specs=[IN_VMEM],
        out_shape=jax.ShapeDtypeStruct((count, piece, cells), pieces.dtype),
    )(pieces)


def couple(kq, lines, twins, others, bands, modes, per_step):
    parts = len(others)
    half = parts // 2
    cells = others[0].shape[1]
    wide = parts * cells
    rows = 2 * bands
    share = lines.shape[1] - rows

    def kernel(kq_ref, lines_ref, twins_ref, *refs):
        other_refs = refs[:parts]
        out_ref = refs[parts]
        wave_re, wave_im, pots, left, right_a, right_b = refs[parts + 1 :]
        step = pl.program_id(0)
        first = lax.axis_index("c") * (share // 2)

        def fill(mode, right):
            for p in range(parts):
                at = slice(p * cells, (p + 1) * cells)
                dv_re = pots[pl.ds(first + 2 * mode, 1), at]
                dv_im = pots[pl.ds(first + 2 * mode + 1, 1), at]
                w_re, w_im = wave_re[:, at], wave_im[:, at]
                right[:bands, at] = (dv_re * w_re - dv_im * w_im).astype(jnp.bfloat16)
                right[bands:, at] = (dv_re * w_im + dv_im * w_re).astype(jnp.bfloat16)

        def finish(slot, right):
            full = lax.dot_general(left[...], right[...], (((1,), (1,)), ((), ())), preferred_element_type=jnp.float32)
            out_ref[slot, 0] = full[:bands, :bands] + full[bands:, bands:]
            out_ref[slot, 1] = full[:bands, bands:] - full[bands:, :bands]

        @pl.when(step == 0)
        def _():
            zl = lax.axis_index("zl")
            crossed = kq_ref[0] // 16 != lax.axis_index("zh")
            for p in range(parts):
                at = slice(p * cells, (p + 1) * cells)
                s = STEPS[p % half]
                turned = lax.rem(2 * zl + 5 - s, 4)
                turned = jnp.where(turned == 2, 3, jnp.where(turned == 3, 2, turned))
                index = jnp.where(crossed, turned, p % half)
                source = lines_ref if p < half else twins_ref
                wave_re[:, at] = source[index, :bands].astype(jnp.float32)
                wave_im[:, at] = source[index, bands:rows].astype(jnp.float32)
                pots[:, at] = source[index, rows:].astype(jnp.float32)
                left[:, at] = other_refs[p][...]

        for j in range(0, per_step, 2):
            fill(step * per_step + j, right_a)
            fill(step * per_step + j + 1, right_b)
            finish(j, right_a)
            finish(j + 1, right_b)

    whole = lambda a: pl.BlockSpec(a.shape, lambda i: (0,) * a.ndim)
    return pl.pallas_call(
        kernel,
        grid=(modes // per_step,),
        in_specs=[IN_SMEM] + [whole(a) for a in (lines, twins, *others)],
        out_specs=pl.BlockSpec((per_step, 2, bands, bands), lambda i: (i, 0, 0, 0)),
        out_shape=jax.ShapeDtypeStruct((modes, 2, bands, bands), jnp.float32),
        scratch_shapes=[
            pltpu.VMEM((bands, wide), jnp.float32),
            pltpu.VMEM((bands, wide), jnp.float32),
            pltpu.VMEM((share, wide), jnp.float32),
            pltpu.VMEM((rows, wide), jnp.bfloat16),
            pltpu.VMEM((rows, wide), jnp.bfloat16),
            pltpu.VMEM((rows, wide), jnp.bfloat16),
        ],
        compiler_params=pltpu.CompilerParams(dimension_semantics=("arbitrary",)),
    )(kq, lines, twins, *others)


def body(psi, dvscf, kq_map):
    bands, cells = psi.shape[2], psi.shape[3]
    modes = dvscf.shape[0] // 8
    slab = psi.reshape(2 * bands, cells)

    swapped = lax.ppermute(slab, ("zh", "zl"), MIRROR)
    packs = pack_lines(slab, dvscf)
    lines = [packs[0]] + [lax.ppermute(packs[i], "zl", ring(STEPS[i])) for i in (1, 2, 3)]
    lines = jnp.stack(lines)
    twins = lax.ppermute(lines, "c", SWAP)

    pieces = pack_spread(slab, swapped, kq_map)
    pieces = lax.all_to_all(pieces, XY, 0, 0, tiled=True)
    phi = lax.all_to_all(choose(pieces), XY, 0, 0, tiled=True).reshape(2 * bands, cells)

    others = [phi] + [lax.ppermute(phi, "zl", ring(STEPS[i])) for i in (1, 2, 3)]
    others += [lax.ppermute(o, "c", SWAP) for o in others]
    out = couple(kq_map, lines, twins, others, bands, modes, 4)
    return out[:, None]


def solution(mesh):
    finer = Mesh(mesh.devices.reshape(2, 4, 4, 4, 2), KA + GA)
    in_specs = (P(KA, None, None, GA), P(None, None, GA), P(KA))
    out_specs = P(GA, KA, None, None, None)
    return jax.shard_map(body, mesh=finer, in_specs=in_specs, out_specs=out_specs, check_vma=False)
```

```python
import jax
import jax.numpy as jnp
from jax import lax
from jax.experimental import pallas as pl
from jax.experimental.pallas import tpu as pltpu
from jax.sharding import Mesh
from jax.sharding import PartitionSpec as P

KA = ("zh", "x", "y")
GA = ("zl", "c")
XY = ("x", "y")
SWAP = [(0, 1), (1, 0)]
MIRROR = [(z, 7 - z) for z in range(8)]
STEPS = (0, 1, 3, 2)
TAG = 8
IN_SMEM = pl.BlockSpec(memory_space=pltpu.SMEM)
IN_VMEM = pl.BlockSpec(memory_space=pltpu.VMEM)


def ring(step, size=4):
    return [(i, (i + step) % size) for i in range(size)]


def send(value, axis, pairs):
    return lax.ppermute(value, axis, pairs)


def pack_lines(slab, potential):
    rows, cells = slab.shape
    modes = potential.shape[0] // 4

    def kernel(slab_ref, pot_ref, *outs):
        zl = lax.axis_index("zl")
        for s, out in zip(STEPS, outs):
            out[:rows] = slab_ref[...]
            first = modes * lax.rem(zl + s, 4)
            for m in range(modes):
                out[rows + 2 * m : rows + 2 * m + 2] = pot_ref[first + m]

    return pl.pallas_call(
        kernel,
        in_specs=[IN_VMEM, IN_VMEM],
        out_shape=[jax.ShapeDtypeStruct((rows + 2 * modes, cells), slab.dtype)] * 4,
    )(slab, potential)


def pack_spread(slab, kq):
    rows, cells = slab.shape
    piece = rows // 16

    def kernel(kq_ref, slab_ref, out):
        tag = jnp.full((TAG, cells), kq_ref[0].astype(jnp.float32)).astype(slab.dtype)
        for j in range(16):
            out[j, :piece] = slab_ref[j * piece : (j + 1) * piece]
            out[j, piece:] = tag

    return pl.pallas_call(
        kernel,
        in_specs=[IN_SMEM, IN_VMEM],
        out_shape=jax.ShapeDtypeStruct((16, piece + TAG, cells), slab.dtype),
    )(kq, slab)


def strip(tagged):
    count, rows, cells = tagged.shape

    def kernel(ref, out):
        out[...] = ref[:, : rows - TAG]

    return pl.pallas_call(
        kernel,
        in_specs=[IN_VMEM],
        out_shape=jax.ShapeDtypeStruct((count, rows - TAG, cells), tagged.dtype),
    )(tagged)


def choose(tagged, swapped):
    count, piece, _ = swapped.shape

    def kernel(ref, swapped_ref, out):
        zh = lax.axis_index("zh")
        for d in range(count):
            source = jnp.max(ref[d, piece:, :128].astype(jnp.float32)).astype(jnp.int32)
            block = lax.rem(source, count)
            here = source // count == zh

            @pl.when(here)
            def _():
                out[d] = ref[block, :piece]

            @pl.when(jnp.logical_not(here))
            def _():
                out[d] = swapped_ref[block]

    return pl.pallas_call(
        kernel,
        in_specs=[IN_VMEM, IN_VMEM],
        out_shape=jax.ShapeDtypeStruct(swapped.shape, swapped.dtype),
    )(tagged, swapped)


def couple(kq, lines, twins, others, bands, modes):
    parts = len(others)
    half = parts // 2
    cells = others[0].shape[1]
    wide = parts * cells
    rows = 2 * bands
    share = lines.shape[1] - rows

    def kernel(kq_ref, lines_ref, twins_ref, *refs):
        other_refs = refs[:parts]
        out_ref = refs[parts]
        wave_re, wave_im, pots, left, right_a, right_b, result, sems = refs[parts + 1 :]
        first = lax.axis_index("c") * (share // 2)
        zl = lax.axis_index("zl")
        crossed = kq_ref[0] // 16 != lax.axis_index("zh")
        for p in range(parts):
            at = slice(p * cells, (p + 1) * cells)
            s = STEPS[p % half]
            turned = lax.rem(2 * zl + 5 - s, 4)
            turned = jnp.where(turned == 2, 3, jnp.where(turned == 3, 2, turned))
            index = jnp.where(crossed, turned, p % half)
            source = lines_ref if p < half else twins_ref
            wave_re[:, at] = source[index, :bands].astype(jnp.float32)
            wave_im[:, at] = source[index, bands:rows].astype(jnp.float32)
            pots[:, at] = source[index, rows:].astype(jnp.float32)
            left[:, at] = other_refs[p][...]

        def fill(mode, right):
            for p in range(parts):
                at = slice(p * cells, (p + 1) * cells)
                dv_re = pots[pl.ds(first + 2 * mode, 1), at]
                dv_im = pots[pl.ds(first + 2 * mode + 1, 1), at]
                w_re, w_im = wave_re[:, at], wave_im[:, at]
                right[:bands, at] = (dv_re * w_re - dv_im * w_im).astype(jnp.bfloat16)
                right[bands:, at] = (dv_re * w_im + dv_im * w_re).astype(jnp.bfloat16)

        def finish(mode, right):
            full = lax.dot_general(left[...], right[...], (((1,), (1,)), ((), ())), preferred_element_type=jnp.float32)
            result[mode, 0] = full[:bands, :bands] + full[bands:, bands:]
            result[mode, 1] = full[:bands, bands:] - full[bands:, :bands]

        def copy(pair):
            return pltpu.make_async_copy(result.at[pl.ds(2 * pair, 2)], out_ref.at[pl.ds(2 * pair, 2)], sems.at[pair])

        fill(0, right_a)

        def pair_step(pair, carry):
            fill(2 * pair + 1, right_b)
            finish(2 * pair, right_a)
            fill(jnp.minimum(2 * pair + 2, modes - 1), right_a)
            finish(2 * pair + 1, right_b)
            copy(pair).start()
            return carry

        lax.fori_loop(0, modes // 2, pair_step, 0)
        for pair in range(modes // 2):
            copy(pair).wait()

    return pl.pallas_call(
        kernel,
        in_specs=[IN_SMEM] + [IN_VMEM] * (2 + parts),
        out_specs=pl.BlockSpec(memory_space=pl.ANY),
        out_shape=jax.ShapeDtypeStruct((modes, 2, bands, bands), jnp.float32),
        scratch_shapes=[
            pltpu.VMEM((bands, wide), jnp.float32),
            pltpu.VMEM((bands, wide), jnp.float32),
            pltpu.VMEM((share, wide), jnp.float32),
            pltpu.VMEM((rows, wide), jnp.bfloat16),
            pltpu.VMEM((rows, wide), jnp.bfloat16),
            pltpu.VMEM((rows, wide), jnp.bfloat16),
            pltpu.VMEM((modes, 2, bands, bands), jnp.float32),
            pltpu.SemaphoreType.DMA((modes // 2,)),
        ],
    )(kq, lines, twins, *others)


def body(psi, dvscf, kq_map):
    bands, cells = psi.shape[2], psi.shape[3]
    modes = dvscf.shape[0] // 8
    slab = psi.reshape(2 * bands, cells)

    tagged = pack_spread(slab, kq_map)
    tagged = lax.all_to_all(tagged, XY, 0, 0, tiled=True)
    swapped = send(strip(tagged), ("zh", "zl"), MIRROR)
    packs = pack_lines(slab, dvscf)
    lines = [packs[0]] + [send(packs[i], "zl", ring(STEPS[i])) for i in (1, 2, 3)]
    lines = jnp.stack(lines)
    twins = send(lines, "c", SWAP)
    chosen = choose(tagged, swapped)
    phi = lax.all_to_all(chosen, XY, 0, 0, tiled=True).reshape(2 * bands, cells)

    others = [phi] + [send(phi, "zl", ring(STEPS[i])) for i in (1, 2, 3)]
    others += [send(o, "c", SWAP) for o in others]
    out = couple(kq_map, lines, twins, others, bands, modes)
    return out[:, None]


def solution(mesh):
    finer = Mesh(mesh.devices.reshape(2, 4, 4, 4, 2), KA + GA)
    in_specs = (P(KA, None, None, GA), P(None, None, GA), P(KA))
    out_specs = P(GA, KA, None, None, None)
    return jax.shard_map(body, mesh=finer, in_specs=in_specs, out_specs=out_specs, check_vma=False)
```

```python
import jax
import jax.numpy as jnp
from jax import lax
from jax.experimental import pallas as pl
from jax.experimental.pallas import tpu as pltpu
from jax.sharding import Mesh
from jax.sharding import PartitionSpec as P

KA = ("zh", "x", "y")
GA = ("zl", "c")
XY = ("x", "y")
SWAP = [(0, 1), (1, 0)]
MIRROR = [(z, 7 - z) for z in range(8)]
STEPS = (0, 1, 3, 2)
TAG = 8
VMEM_LIMIT = 20 * 2**20
IN_SMEM = pl.BlockSpec(memory_space=pltpu.SMEM)
IN_VMEM = pl.BlockSpec(memory_space=pltpu.VMEM)


def ring(step, size=4):
    return [(i, (i + step) % size) for i in range(size)]


def pack_lines(slab, potential):
    rows, cells = slab.shape
    modes = potential.shape[0] // 4

    def kernel(slab_ref, pot_ref, *outs):
        zl = lax.axis_index("zl")
        for s, out in zip(STEPS, outs):
            out[:rows] = slab_ref[...]
            first = modes * lax.rem(zl + s, 4)
            for m in range(modes):
                out[rows + 2 * m : rows + 2 * m + 2] = pot_ref[first + m]

    return pl.pallas_call(
        kernel,
        in_specs=[IN_VMEM, IN_VMEM],
        out_shape=[jax.ShapeDtypeStruct((rows + 2 * modes, cells), slab.dtype)] * 4,
    )(slab, potential)


def pack_spread(slab, swapped, kq):
    rows, cells = slab.shape
    piece = rows // 16

    def kernel(kq_ref, slab_ref, swapped_ref, out):
        tag = jnp.full((TAG, cells), kq_ref[0].astype(jnp.float32)).astype(slab.dtype)
        for j in range(16):
            out[j, :piece] = slab_ref[j * piece : (j + 1) * piece]
            out[j, piece : 2 * piece] = swapped_ref[j * piece : (j + 1) * piece]
            out[j, 2 * piece :] = tag

    return pl.pallas_call(
        kernel,
        in_specs=[IN_SMEM, IN_VMEM, IN_VMEM],
        out_shape=jax.ShapeDtypeStruct((16, 2 * piece + TAG, cells), slab.dtype),
    )(kq, slab, swapped)


def choose(pieces):
    count, rows, cells = pieces.shape
    piece = (rows - TAG) // 2

    def kernel(ref, out):
        zh = lax.axis_index("zh")
        for d in range(count):
            source = jnp.max(ref[d, 2 * piece :, :128].astype(jnp.float32)).astype(jnp.int32)
            side = jnp.where(source // count == zh, 0, piece)
            out[d] = ref[lax.rem(source, count), pl.ds(pl.multiple_of(side, piece), piece), :]

    return pl.pallas_call(
        kernel,
        in_specs=[IN_VMEM],
        out_shape=jax.ShapeDtypeStruct((count, piece, cells), pieces.dtype),
    )(pieces)


def couple(kq, lines, twins, others, bands, modes):
    parts = len(others)
    half = parts // 2
    cells = others[0].shape[1]
    wide = parts * cells
    rows = 2 * bands
    share = lines.shape[1] - rows

    def kernel(kq_ref, lines_ref, twins_ref, *refs):
        other_refs = refs[:parts]
        out_ref = refs[parts]
        wave_re, wave_im, pots, left, right_a, right_b, result, sems = refs[parts + 1 :]
        first = lax.axis_index("c") * (share // 2)
        zl = lax.axis_index("zl")
        crossed = kq_ref[0] // 16 != lax.axis_index("zh")
        for p in range(parts):
            at = slice(p * cells, (p + 1) * cells)
            s = STEPS[p % half]
            turned = lax.rem(2 * zl + 5 - s, 4)
            turned = jnp.where(turned == 2, 3, jnp.where(turned == 3, 2, turned))
            index = jnp.where(crossed, turned, p % half)
            source = lines_ref if p < half else twins_ref
            wave_re[:, at] = source[index, :bands].astype(jnp.float32)
            wave_im[:, at] = source[index, bands:rows].astype(jnp.float32)
            pots[:, at] = source[index, rows:].astype(jnp.float32)
            left[:, at] = other_refs[p][...]

        def fill(mode, right):
            for p in range(parts):
                at = slice(p * cells, (p + 1) * cells)
                dv_re = pots[pl.ds(first + 2 * mode, 1), at]
                dv_im = pots[pl.ds(first + 2 * mode + 1, 1), at]
                w_re, w_im = wave_re[:, at], wave_im[:, at]
                right[:bands, at] = (dv_re * w_re - dv_im * w_im).astype(jnp.bfloat16)
                right[bands:, at] = (dv_re * w_im + dv_im * w_re).astype(jnp.bfloat16)

        def finish(mode, right):
            full = lax.dot_general(left[...], right[...], (((1,), (1,)), ((), ())), preferred_element_type=jnp.float32)
            result[mode, 0] = full[:bands, :bands] + full[bands:, bands:]
            result[mode, 1] = full[:bands, bands:] - full[bands:, :bands]

        def copy(pair):
            return pltpu.make_async_copy(result.at[pl.ds(2 * pair, 2)], out_ref.at[pl.ds(2 * pair, 2)], sems.at[pair])

        fill(0, right_a)

        def pair_step(pair, carry):
            fill(2 * pair + 1, right_b)
            finish(2 * pair, right_a)
            fill(jnp.minimum(2 * pair + 2, modes - 1), right_a)
            finish(2 * pair + 1, right_b)
            copy(pair).start()
            return carry

        lax.fori_loop(0, modes // 2, pair_step, 0)
        for pair in range(modes // 2):
            copy(pair).wait()

    return pl.pallas_call(
        kernel,
        in_specs=[IN_SMEM] + [IN_VMEM] * (2 + parts),
        out_specs=pl.BlockSpec(memory_space=pl.ANY),
        out_shape=jax.ShapeDtypeStruct((modes, 2, bands, bands), jnp.float32),
        scratch_shapes=[
            pltpu.VMEM((bands, wide), jnp.float32),
            pltpu.VMEM((bands, wide), jnp.float32),
            pltpu.VMEM((share, wide), jnp.float32),
            pltpu.VMEM((rows, wide), jnp.bfloat16),
            pltpu.VMEM((rows, wide), jnp.bfloat16),
            pltpu.VMEM((rows, wide), jnp.bfloat16),
            pltpu.VMEM((modes, 2, bands, bands), jnp.float32),
            pltpu.SemaphoreType.DMA((modes // 2,)),
        ],
        compiler_params=pltpu.CompilerParams(vmem_limit_bytes=VMEM_LIMIT),
    )(kq, lines, twins, *others)


def body(psi, dvscf, kq_map):
    bands, cells = psi.shape[2], psi.shape[3]
    modes = dvscf.shape[0] // 8
    slab = psi.reshape(2 * bands, cells)

    swapped = lax.ppermute(slab, ("zh", "zl"), MIRROR)
    packs = pack_lines(slab, dvscf)
    lines = [packs[0]] + [lax.ppermute(packs[i], "zl", ring(STEPS[i])) for i in (1, 2, 3)]
    lines = jnp.stack(lines)
    twins = lax.ppermute(lines, "c", SWAP)

    pieces = pack_spread(slab, swapped, kq_map)
    pieces = lax.all_to_all(pieces, XY, 0, 0, tiled=True)
    phi = lax.all_to_all(choose(pieces), XY, 0, 0, tiled=True).reshape(2 * bands, cells)

    others = [phi] + [lax.ppermute(phi, "zl", ring(STEPS[i])) for i in (1, 2, 3)]
    others += [lax.ppermute(o, "c", SWAP) for o in others]
    out = couple(kq_map, lines, twins, others, bands, modes)
    return out[:, None]


def solution(mesh):
    finer = Mesh(mesh.devices.reshape(2, 4, 4, 4, 2), KA + GA)
    in_specs = (P(KA, None, None, GA), P(None, None, GA), P(KA))
    out_specs = P(GA, KA, None, None, None)
    return jax.shard_map(body, mesh=finer, in_specs=in_specs, out_specs=out_specs, check_vma=False)
```

```python
import jax
import jax.numpy as jnp
from jax import lax
from jax.experimental import pallas as pl
from jax.experimental.pallas import tpu as pltpu
from jax.sharding import Mesh
from jax.sharding import PartitionSpec as P

KA = ("zh", "x", "y")
GA = ("zl", "c")
XY = ("x", "y")
SWAP = [(0, 1), (1, 0)]
MIRROR = [(z, 7 - z) for z in range(8)]
STEPS = (0, 1, 3, 2)
TAG = 8
SMALL = pltpu.CompilerParams(vmem_limit_bytes=20 * 2**20)
IN_SMEM = pl.BlockSpec(memory_space=pltpu.SMEM)
IN_VMEM = pl.BlockSpec(memory_space=pltpu.VMEM)


def ring(step, size=4):
    return [(i, (i + step) % size) for i in range(size)]


def pack_lines(slab, potential):
    rows, cells = slab.shape
    modes = potential.shape[0] // 4

    def kernel(slab_ref, pot_ref, *outs):
        zl = lax.axis_index("zl")
        for s, out in zip(STEPS, outs):
            out[:rows] = slab_ref[...]
            first = modes * lax.rem(zl + s, 4)
            for m in range(modes):
                out[rows + 2 * m : rows + 2 * m + 2] = pot_ref[first + m]

    return pl.pallas_call(
        kernel,
        in_specs=[IN_VMEM, IN_VMEM],
        out_shape=[jax.ShapeDtypeStruct((rows + 2 * modes, cells), slab.dtype)] * 4,
        compiler_params=SMALL,
    )(slab, potential)


def pack_spread(slab, kq):
    rows, cells = slab.shape
    piece = rows // 16

    def kernel(kq_ref, slab_ref, out):
        tag = jnp.full((TAG, cells), kq_ref[0].astype(jnp.float32)).astype(slab.dtype)
        for j in range(16):
            out[j, :piece] = slab_ref[j * piece : (j + 1) * piece]
            out[j, piece:] = tag

    return pl.pallas_call(
        kernel,
        in_specs=[IN_SMEM, IN_VMEM],
        out_shape=jax.ShapeDtypeStruct((16, piece + TAG, cells), slab.dtype),
        compiler_params=SMALL,
    )(kq, slab)


def strip(tagged):
    count, rows, cells = tagged.shape

    def kernel(ref, out):
        out[...] = ref[:, : rows - TAG]

    return pl.pallas_call(
        kernel,
        in_specs=[IN_VMEM],
        out_shape=jax.ShapeDtypeStruct((count, rows - TAG, cells), tagged.dtype),
        compiler_params=SMALL,
    )(tagged)


def choose(tagged, swapped):
    count, piece, _ = swapped.shape

    def kernel(ref, swapped_ref, out):
        zh = lax.axis_index("zh")
        for d in range(count):
            source = jnp.max(ref[d, piece:, :128].astype(jnp.float32)).astype(jnp.int32)
            block = lax.rem(source, count)
            out[d] = jnp.where(source // count == zh, ref[block, :piece], swapped_ref[block])

    return pl.pallas_call(
        kernel,
        in_specs=[IN_VMEM, IN_VMEM],
        out_shape=jax.ShapeDtypeStruct(swapped.shape, swapped.dtype),
        compiler_params=SMALL,
    )(tagged, swapped)


def couple(kq, lines, twins, others, steps, bands, modes, last, before=None):
    parts = len(others)
    half = parts // 2
    cells = others[0].shape[1]
    wide = parts * cells
    rows = 2 * bands
    share = lines.shape[1] - rows
    pairs = modes // 2

    def kernel(kq_ref, lines_ref, twins_ref, *refs):
        other_refs, refs = refs[:parts], refs[parts:]
        if before is not None:
            before_ref, *refs = refs
        out_ref, wave_re, wave_im, pots, left, right_a, right_b, *more = refs
        result, sems = more if last else (out_ref, None)

        def copy(pair):
            at = pl.ds(2 * pair, 2)
            return pltpu.make_async_copy(result.at[at], out_ref.at[at], sems.at[pair])

        first = lax.axis_index("c") * (share // 2)
        zl = lax.axis_index("zl")
        crossed = kq_ref[0] // 16 != lax.axis_index("zh")
        for p in range(parts):
            at = slice(p * cells, (p + 1) * cells)
            s = steps[p % half]
            turned = lax.rem(2 * zl + 5 - s, 4)
            turned = jnp.where(turned == 2, 3, jnp.where(turned == 3, 2, turned))
            index = jnp.where(crossed, turned, STEPS.index(s))
            source = lines_ref if p < half else twins_ref
            wave_re[:, at] = source[index, :bands].astype(jnp.float32)
            wave_im[:, at] = source[index, bands:rows].astype(jnp.float32)
            pots[:, at] = source[index, rows:].astype(jnp.float32)
            left[:, at] = other_refs[p][...]

        def fill(mode, right):
            for p in range(parts):
                at = slice(p * cells, (p + 1) * cells)
                dv_re = pots[pl.ds(first + 2 * mode, 1), at]
                dv_im = pots[pl.ds(first + 2 * mode + 1, 1), at]
                w_re, w_im = wave_re[:, at], wave_im[:, at]
                right[:bands, at] = (dv_re * w_re - dv_im * w_im).astype(jnp.bfloat16)
                right[bands:, at] = (dv_re * w_im + dv_im * w_re).astype(jnp.bfloat16)

        def finish(mode, right):
            full = lax.dot_general(left[...], right[...], (((1,), (1,)), ((), ())), preferred_element_type=jnp.float32)
            real = full[:bands, :bands] + full[bands:, bands:]
            imag = full[:bands, bands:] - full[bands:, :bands]
            if before is not None:
                real, imag = real + before_ref[mode, 0], imag + before_ref[mode, 1]
            result[mode, 0] = real
            result[mode, 1] = imag

        fill(0, right_a)
        for pair in range(pairs):
            fill(2 * pair + 1, right_b)
            finish(2 * pair, right_a)
            if pair + 1 < pairs:
                fill(2 * pair + 2, right_a)
            finish(2 * pair + 1, right_b)
            if last:
                copy(pair).start()
        if last:
            for pair in range(pairs):
                copy(pair).wait()

    total = (modes, 2, bands, bands)
    scratch = [
        pltpu.VMEM((bands, wide), jnp.float32),
        pltpu.VMEM((bands, wide), jnp.float32),
        pltpu.VMEM((share, wide), jnp.float32),
        pltpu.VMEM((rows, wide), jnp.bfloat16),
        pltpu.VMEM((rows, wide), jnp.bfloat16),
        pltpu.VMEM((rows, wide), jnp.bfloat16),
    ]
    if last:
        scratch += [pltpu.VMEM(total, jnp.float32), pltpu.SemaphoreType.DMA((pairs,))]
    args = [kq, lines, twins, *others]
    specs = [IN_SMEM] + [IN_VMEM] * (2 + parts)
    if before is not None:
        args, specs = args + [before], specs + [IN_VMEM]
    return pl.pallas_call(
        kernel,
        in_specs=specs,
        out_specs=pl.BlockSpec(memory_space=pl.ANY) if last else IN_VMEM,
        out_shape=jax.ShapeDtypeStruct(total, jnp.float32),
        scratch_shapes=scratch,
        compiler_params=SMALL,
    )(*args)


def body(psi, dvscf, kq_map):
    bands, cells = psi.shape[2], psi.shape[3]
    modes = dvscf.shape[0] // 8
    slab = psi.reshape(2 * bands, cells)

    tagged = pack_spread(slab, kq_map)
    tagged = lax.all_to_all(tagged, XY, 0, 0, tiled=True)
    packs = pack_lines(slab, dvscf)
    lines = [packs[0]] + [lax.ppermute(packs[i], "zl", ring(STEPS[i])) for i in (1, 2, 3)]
    lines = jnp.stack(lines)
    twins = lax.ppermute(lines, "c", SWAP)
    swapped = lax.ppermute(strip(tagged), ("zh", "zl"), MIRROR)
    phi = lax.all_to_all(choose(tagged, swapped), XY, 0, 0, tiled=True).reshape(2 * bands, cells)

    others = [phi] + [lax.ppermute(phi, "zl", ring(STEPS[i])) for i in (1, 2, 3)]
    mates = [lax.ppermute(o, "c", SWAP) for o in others]
    out = couple(kq_map, lines, twins, others[:1] + mates[:1], STEPS[:1], bands, modes, False)
    out = couple(kq_map, lines, twins, others[1:] + mates[1:], STEPS[1:], bands, modes, True, out)
    return out[:, None]


def solution(mesh):
    finer = Mesh(mesh.devices.reshape(2, 4, 4, 4, 2), KA + GA)
    in_specs = (P(KA, None, None, GA), P(None, None, GA), P(KA))
    out_specs = P(GA, KA, None, None, None)
    return jax.shard_map(body, mesh=finer, in_specs=in_specs, out_specs=out_specs, check_vma=False)
```

```python
import jax
import jax.numpy as jnp
from jax import lax
from jax.experimental import pallas as pl
from jax.experimental.pallas import tpu as pltpu
from jax.sharding import Mesh
from jax.sharding import PartitionSpec as P

KA = ("zh", "x", "y")
GA = ("zl", "c")
XY = ("x", "y")
SWAP = [(0, 1), (1, 0)]
MIRROR = [(z, 7 - z) for z in range(8)]
STEPS = (0, 1, 3, 2)
TAG = 8
SMALL = pltpu.CompilerParams(vmem_limit_bytes=20 * 2**20)
IN_SMEM = pl.BlockSpec(memory_space=pltpu.SMEM)
IN_HBM = pl.BlockSpec(memory_space=pltpu.HBM)
IN_VMEM = pl.BlockSpec(memory_space=pltpu.VMEM)


def ring(step, size=4):
    return [(i, (i + step) % size) for i in range(size)]


def pack_lines(slab, potential):
    rows, cells = slab.shape
    modes = potential.shape[0] // 4

    def kernel(slab_ref, pot_ref, *outs):
        zl = lax.axis_index("zl")
        for s, out in zip(STEPS, outs):
            out[:rows] = slab_ref[...]
            first = modes * lax.rem(zl + s, 4)
            for m in range(modes):
                out[rows + 2 * m : rows + 2 * m + 2] = pot_ref[first + m]

    return pl.pallas_call(
        kernel,
        in_specs=[IN_VMEM, IN_VMEM],
        out_shape=[jax.ShapeDtypeStruct((rows + 2 * modes, cells), slab.dtype)] * 4,
        compiler_params=SMALL,
    )(slab, potential)


def pack_spread(slab, kq):
    rows, cells = slab.shape
    piece = rows // 16

    def kernel(kq_ref, slab_ref, out, tags, sems):
        body = pltpu.make_async_copy(slab_ref, out.at[:, :piece], sems.at[0])
        body.start()
        tags[...] = jnp.full(tags.shape, kq_ref[0].astype(jnp.float32)).astype(slab.dtype)
        tail = pltpu.make_async_copy(tags, out.at[:, piece:], sems.at[1])
        tail.start()
        body.wait()
        tail.wait()

    return pl.pallas_call(
        kernel,
        in_specs=[IN_SMEM, IN_HBM],
        out_specs=IN_HBM,
        out_shape=jax.ShapeDtypeStruct((16, piece + TAG, cells), slab.dtype),
        scratch_shapes=[pltpu.VMEM((16, TAG, cells), slab.dtype), pltpu.SemaphoreType.DMA((2,))],
    )(kq, slab.reshape(16, piece, cells))


def strip(tagged):
    count, rows, cells = tagged.shape

    def kernel(ref, out):
        out[...] = ref[:, : rows - TAG]

    return pl.pallas_call(
        kernel,
        in_specs=[IN_VMEM],
        out_shape=jax.ShapeDtypeStruct((count, rows - TAG, cells), tagged.dtype),
        compiler_params=SMALL,
    )(tagged)


def choose(tagged, swapped):
    count, piece, _ = swapped.shape

    def kernel(ref, swapped_ref, out):
        zh = lax.axis_index("zh")
        for d in range(count):
            source = jnp.max(ref[d, piece:, :128].astype(jnp.float32)).astype(jnp.int32)
            block = lax.rem(source, count)
            out[d] = jnp.where(source // count == zh, ref[block, :piece], swapped_ref[block])

    return pl.pallas_call(
        kernel,
        in_specs=[IN_VMEM, IN_VMEM],
        out_shape=jax.ShapeDtypeStruct(swapped.shape, swapped.dtype),
        compiler_params=SMALL,
    )(tagged, swapped)


def couple(kq, lines, twins, others, steps, bands, modes, last, before=None):
    parts = len(others)
    half = parts // 2
    cells = others[0].shape[1]
    wide = parts * cells
    rows = 2 * bands
    share = lines.shape[1] - rows
    pairs = modes // 2

    def kernel(kq_ref, lines_ref, twins_ref, *refs):
        other_refs, refs = refs[:parts], refs[parts:]
        if before is not None:
            before_ref, *refs = refs
        out_ref, wave_re, wave_im, pots, left, right_a, right_b, *more = refs
        result, sems = more if last else (out_ref, None)

        def copy(pair):
            at = pl.ds(2 * pair, 2)
            return pltpu.make_async_copy(result.at[at], out_ref.at[at], sems.at[pair])

        first = lax.axis_index("c") * (share // 2)
        zl = lax.axis_index("zl")
        crossed = kq_ref[0] // 16 != lax.axis_index("zh")
        for p in range(parts):
            at = slice(p * cells, (p + 1) * cells)
            s = steps[p % half]
            turned = lax.rem(2 * zl + 5 - s, 4)
            turned = jnp.where(turned == 2, 3, jnp.where(turned == 3, 2, turned))
            index = jnp.where(crossed, turned, STEPS.index(s))
            source = lines_ref if p < half else twins_ref
            wave_re[:, at] = source[index, :bands].astype(jnp.float32)
            wave_im[:, at] = source[index, bands:rows].astype(jnp.float32)
            pots[:, at] = source[index, rows:].astype(jnp.float32)
            left[:, at] = other_refs[p][...]

        def fill(mode, right):
            for p in range(parts):
                at = slice(p * cells, (p + 1) * cells)
                dv_re = pots[pl.ds(first + 2 * mode, 1), at]
                dv_im = pots[pl.ds(first + 2 * mode + 1, 1), at]
                w_re, w_im = wave_re[:, at], wave_im[:, at]
                right[:bands, at] = (dv_re * w_re - dv_im * w_im).astype(jnp.bfloat16)
                right[bands:, at] = (dv_re * w_im + dv_im * w_re).astype(jnp.bfloat16)

        def finish(mode, right):
            full = lax.dot_general(left[...], right[...], (((1,), (1,)), ((), ())), preferred_element_type=jnp.float32)
            real = full[:bands, :bands] + full[bands:, bands:]
            imag = full[:bands, bands:] - full[bands:, :bands]
            if before is not None:
                real, imag = real + before_ref[mode, 0], imag + before_ref[mode, 1]
            result[mode, 0] = real
            result[mode, 1] = imag

        fill(0, right_a)
        for pair in range(pairs):
            fill(2 * pair + 1, right_b)
            finish(2 * pair, right_a)
            if pair + 1 < pairs:
                fill(2 * pair + 2, right_a)
            finish(2 * pair + 1, right_b)
            if last:
                copy(pair).start()
        if last:
            for pair in range(pairs):
                copy(pair).wait()

    total = (modes, 2, bands, bands)
    scratch = [
        pltpu.VMEM((bands, wide), jnp.float32),
        pltpu.VMEM((bands, wide), jnp.float32),
        pltpu.VMEM((share, wide), jnp.float32),
        pltpu.VMEM((rows, wide), jnp.bfloat16),
        pltpu.VMEM((rows, wide), jnp.bfloat16),
        pltpu.VMEM((rows, wide), jnp.bfloat16),
    ]
    if last:
        scratch += [pltpu.VMEM(total, jnp.float32), pltpu.SemaphoreType.DMA((pairs,))]
    args = [kq, lines, twins, *others]
    specs = [IN_SMEM] + [IN_VMEM] * (2 + parts)
    if before is not None:
        args, specs = args + [before], specs + [IN_VMEM]
    return pl.pallas_call(
        kernel,
        in_specs=specs,
        out_specs=IN_HBM if last else IN_VMEM,
        out_shape=jax.ShapeDtypeStruct(total, jnp.float32),
        scratch_shapes=scratch,
        compiler_params=SMALL,
    )(*args)


def body(psi, dvscf, kq_map):
    bands, cells = psi.shape[2], psi.shape[3]
    modes = dvscf.shape[0] // 8
    slab = psi.reshape(2 * bands, cells)

    tagged = pack_spread(slab, kq_map)
    tagged = lax.all_to_all(tagged, XY, 0, 0, tiled=True)
    packs = pack_lines(slab, dvscf)
    lines = [packs[0]] + [lax.ppermute(packs[i], "zl", ring(STEPS[i])) for i in (1, 2, 3)]
    lines = jnp.stack(lines)
    twins = lax.ppermute(lines, "c", SWAP)
    swapped = lax.ppermute(strip(tagged), ("zh", "zl"), MIRROR)
    phi = lax.all_to_all(choose(tagged, swapped), XY, 0, 0, tiled=True).reshape(2 * bands, cells)

    others = [phi] + [lax.ppermute(phi, "zl", ring(STEPS[i])) for i in (1, 2, 3)]
    mates = [lax.ppermute(o, "c", SWAP) for o in others]
    out = couple(kq_map, lines, twins, others[:1] + mates[:1], STEPS[:1], bands, modes, False)
    out = couple(kq_map, lines, twins, others[1:] + mates[1:], STEPS[1:], bands, modes, True, out)
    return out[:, None]


def solution(mesh):
    finer = Mesh(mesh.devices.reshape(2, 4, 4, 4, 2), KA + GA)
    in_specs = (P(KA, None, None, GA), P(None, None, GA), P(KA))
    out_specs = P(GA, KA, None, None, None)
    return jax.shard_map(body, mesh=finer, in_specs=in_specs, out_specs=out_specs, check_vma=False)
```

```python
import jax
import jax.numpy as jnp
from jax import lax
from jax.experimental import pallas as pl
from jax.experimental.pallas import tpu as pltpu
from jax.sharding import Mesh
from jax.sharding import PartitionSpec as P

KA = ("zh", "x", "y")
GA = ("zl", "c")
XY = ("x", "y")
SWAP = [(0, 1), (1, 0)]
MIRROR = [(z, 7 - z) for z in range(8)]
STEPS = (0, 1, 3, 2)
TAG = 8
SMALL = pltpu.CompilerParams(vmem_limit_bytes=20 * 2**20)
IN_SMEM = pl.BlockSpec(memory_space=pltpu.SMEM)
IN_VMEM = pl.BlockSpec(memory_space=pltpu.VMEM)


def ring(step, size=4):
    return [(i, (i + step) % size) for i in range(size)]


def pack_lines(slab, potential):
    rows, cells = slab.shape
    modes = potential.shape[0] // 4

    def kernel(slab_ref, pot_ref, *outs):
        zl = lax.axis_index("zl")
        for s, out in zip(STEPS, outs):
            out[:rows] = slab_ref[...]
            first = modes * lax.rem(zl + s, 4)
            for m in range(modes):
                out[rows + 2 * m : rows + 2 * m + 2] = pot_ref[first + m]

    return pl.pallas_call(
        kernel,
        in_specs=[IN_VMEM, IN_VMEM],
        out_shape=[jax.ShapeDtypeStruct((rows + 2 * modes, cells), slab.dtype)] * 4,
        compiler_params=SMALL,
    )(slab, potential)


def pack_spread(slab, swapped, kq):
    rows, cells = slab.shape
    piece = rows // 16

    def kernel(kq_ref, slab_ref, swapped_ref, out):
        tag = jnp.full((TAG, cells), kq_ref[0].astype(jnp.float32)).astype(slab.dtype)
        for j in range(16):
            out[j, :piece] = slab_ref[j * piece : (j + 1) * piece]
            out[j, piece : 2 * piece] = swapped_ref[j * piece : (j + 1) * piece]
            out[j, 2 * piece :] = tag

    return pl.pallas_call(
        kernel,
        in_specs=[IN_SMEM, IN_VMEM, IN_VMEM],
        out_shape=jax.ShapeDtypeStruct((16, 2 * piece + TAG, cells), slab.dtype),
        compiler_params=SMALL,
    )(kq, slab, swapped)


def choose(pieces):
    count, rows, cells = pieces.shape
    piece = (rows - TAG) // 2

    def kernel(ref, out):
        zh = lax.axis_index("zh")
        for d in range(count):
            source = jnp.max(ref[d, 2 * piece :, :128].astype(jnp.float32)).astype(jnp.int32)
            side = jnp.where(source // count == zh, 0, piece)
            out[d] = ref[lax.rem(source, count), pl.ds(pl.multiple_of(side, piece), piece), :]

    return pl.pallas_call(
        kernel,
        in_specs=[IN_VMEM],
        out_shape=jax.ShapeDtypeStruct((count, piece, cells), pieces.dtype),
        compiler_params=SMALL,
    )(pieces)


def couple(kq, lines, twins, others, steps, bands, modes, last, before=None):
    parts = len(others)
    half = parts // 2
    cells = others[0].shape[1]
    wide = parts * cells
    rows = 2 * bands
    share = lines.shape[1] - rows
    pairs = modes // 2

    def kernel(kq_ref, lines_ref, twins_ref, *refs):
        other_refs, refs = refs[:parts], refs[parts:]
        if before is not None:
            before_ref, *refs = refs
        out_ref, wave_re, wave_im, pots, left, right_a, right_b, *more = refs
        result, sems = more if last else (out_ref, None)

        def copy(pair):
            at = pl.ds(2 * pair, 2)
            return pltpu.make_async_copy(result.at[at], out_ref.at[at], sems.at[pair])

        first = lax.axis_index("c") * (share // 2)
        zl = lax.axis_index("zl")
        crossed = kq_ref[0] // 16 != lax.axis_index("zh")
        for p in range(parts):
            at = slice(p * cells, (p + 1) * cells)
            s = steps[p % half]
            turned = lax.rem(2 * zl + 5 - s, 4)
            turned = jnp.where(turned == 2, 3, jnp.where(turned == 3, 2, turned))
            index = jnp.where(crossed, turned, STEPS.index(s))
            source = lines_ref if p < half else twins_ref
            wave_re[:, at] = source[index, :bands].astype(jnp.float32)
            wave_im[:, at] = source[index, bands:rows].astype(jnp.float32)
            pots[:, at] = source[index, rows:].astype(jnp.float32)
            left[:, at] = other_refs[p][...]

        def fill(mode, right):
            for p in range(parts):
                at = slice(p * cells, (p + 1) * cells)
                dv_re = pots[pl.ds(first + 2 * mode, 1), at]
                dv_im = pots[pl.ds(first + 2 * mode + 1, 1), at]
                w_re, w_im = wave_re[:, at], wave_im[:, at]
                right[:bands, at] = (dv_re * w_re - dv_im * w_im).astype(jnp.bfloat16)
                right[bands:, at] = (dv_re * w_im + dv_im * w_re).astype(jnp.bfloat16)

        def finish(mode, right):
            full = lax.dot_general(left[...], right[...], (((1,), (1,)), ((), ())), preferred_element_type=jnp.float32)
            real = full[:bands, :bands] + full[bands:, bands:]
            imag = full[:bands, bands:] - full[bands:, :bands]
            if before is not None:
                real, imag = real + before_ref[mode, 0], imag + before_ref[mode, 1]
            result[mode, 0] = real
            result[mode, 1] = imag

        fill(0, right_a)
        for pair in range(pairs):
            fill(2 * pair + 1, right_b)
            finish(2 * pair, right_a)
            if pair + 1 < pairs:
                fill(2 * pair + 2, right_a)
            finish(2 * pair + 1, right_b)
            if last:
                copy(pair).start()
        if last:
            for pair in range(pairs):
                copy(pair).wait()

    total = (modes, 2, bands, bands)
    scratch = [
        pltpu.VMEM((bands, wide), jnp.float32),
        pltpu.VMEM((bands, wide), jnp.float32),
        pltpu.VMEM((share, wide), jnp.float32),
        pltpu.VMEM((rows, wide), jnp.bfloat16),
        pltpu.VMEM((rows, wide), jnp.bfloat16),
        pltpu.VMEM((rows, wide), jnp.bfloat16),
    ]
    if last:
        scratch += [pltpu.VMEM(total, jnp.float32), pltpu.SemaphoreType.DMA((pairs,))]
    args = [kq, lines, twins, *others]
    specs = [IN_SMEM] + [IN_VMEM] * (2 + parts)
    if before is not None:
        args, specs = args + [before], specs + [IN_VMEM]
    return pl.pallas_call(
        kernel,
        in_specs=specs,
        out_specs=pl.BlockSpec(memory_space=pl.ANY) if last else IN_VMEM,
        out_shape=jax.ShapeDtypeStruct(total, jnp.float32),
        scratch_shapes=scratch,
        compiler_params=SMALL,
    )(*args)


def body(psi, dvscf, kq_map):
    bands, cells = psi.shape[2], psi.shape[3]
    modes = dvscf.shape[0] // 8
    slab = psi.reshape(2 * bands, cells)

    swapped = lax.ppermute(slab, ("zh", "zl"), MIRROR)
    packs = pack_lines(slab, dvscf)
    pieces = lax.all_to_all(pack_spread(slab, swapped, kq_map), XY, 0, 0, tiled=True)
    lines = [packs[0]] + [lax.ppermute(packs[i], "zl", ring(STEPS[i])) for i in (1, 2, 3)]
    lines = jnp.stack(lines)
    twins = lax.ppermute(lines, "c", SWAP)
    phi = lax.all_to_all(choose(pieces), XY, 0, 0, tiled=True).reshape(2 * bands, cells)

    others = [phi] + [lax.ppermute(phi, "zl", ring(STEPS[i])) for i in (1, 2, 3)]
    mates = [lax.ppermute(o, "c", SWAP) for o in others]
    out = None
    for name, at in (("early", slice(0, 1)), ("middle", slice(1, 3)), ("late", slice(3, 4))):
        out = couple(kq_map, lines, twins, others[at] + mates[at], STEPS[at], bands, modes, name == "late", out)
    return out[:, None]


def solution(mesh):
    finer = Mesh(mesh.devices.reshape(2, 4, 4, 4, 2), KA + GA)
    in_specs = (P(KA, None, None, GA), P(None, None, GA), P(KA))
    out_specs = P(GA, KA, None, None, None)
    return jax.shard_map(body, mesh=finer, in_specs=in_specs, out_specs=out_specs, check_vma=False)
```

```python
import jax
import jax.numpy as jnp
from jax import lax
from jax.experimental import pallas as pl
from jax.experimental.pallas import tpu as pltpu
from jax.sharding import Mesh
from jax.sharding import PartitionSpec as P

KA = ("zh", "x", "y")
GA = ("zl", "c")
SWAP = [(0, 1), (1, 0)]
MIRROR = [(z, 7 - z) for z in range(8)]
STEPS = (0, 1, 3, 2)
SMALL = pltpu.CompilerParams(vmem_limit_bytes=20 * 2**20)
IN_SMEM = pl.BlockSpec(memory_space=pltpu.SMEM)
IN_VMEM = pl.BlockSpec(memory_space=pltpu.VMEM)


def ring(step, size=4):
    return [(i, (i + step) % size) for i in range(size)]


def pack_lines(slab, potential):
    rows, cells = slab.shape
    modes = potential.shape[0] // 4

    def kernel(slab_ref, pot_ref, *outs):
        zl = lax.axis_index("zl")
        for s, out in zip(STEPS, outs):
            out[:rows] = slab_ref[...]
            first = modes * lax.rem(zl + s, 4)
            for m in range(modes):
                out[rows + 2 * m : rows + 2 * m + 2] = pot_ref[first + m]

    return pl.pallas_call(
        kernel,
        in_specs=[IN_VMEM, IN_VMEM],
        out_shape=[jax.ShapeDtypeStruct((rows + 2 * modes, cells), slab.dtype)] * 4,
        compiler_params=SMALL,
    )(slab, potential)


def number_in(ref):
    return jnp.max(ref[...].astype(jnp.float32)).astype(jnp.int32)


def pick(number, values):
    out = values[0]
    for i, value in enumerate(values[1:], 1):
        out = jnp.where(number == i, value, out)
    return out


def choose(wanted, blocks):
    count = len(wanted)
    rows, cells = blocks[0].shape

    def kernel(*refs):
        numbers = [number_in(ref) for ref in refs[:count]]
        held, outs = refs[count : count + len(blocks)], refs[count + len(blocks) :]
        zh, y = lax.axis_index("zh"), lax.axis_index("y")
        places = []
        for number in numbers:
            back = lax.rem(y + 4 - lax.rem(number, 4), 4)
            back = jnp.where(back == 2, 3, jnp.where(back == 3, 2, back))
            places.append(jnp.where(number // 16 == zh, back, back + 4))
        for at in range(0, rows, 16):
            values = [ref[at : at + 16] for ref in held]
            for place, out in zip(places, outs):
                out[at : at + 16] = pick(place, values)

    return pl.pallas_call(
        kernel,
        in_specs=[IN_VMEM] * (count + len(blocks)),
        out_shape=[jax.ShapeDtypeStruct((rows, cells), blocks[0].dtype)] * count,
        compiler_params=SMALL,
    )(*wanted, *blocks)


def keep(own, came):
    rows, cells = came[0].shape

    def kernel(own_ref, *refs):
        number = number_in(own_ref)
        back = lax.rem(lax.axis_index("x") + 4 - lax.rem(number // 4, 4), 4)
        back = jnp.where(back == 2, 3, jnp.where(back == 3, 2, back))
        for at in range(0, rows, 16):
            refs[-1][at : at + 16] = pick(back, [ref[at : at + 16] for ref in refs[:-1]])

    return pl.pallas_call(
        kernel,
        in_specs=[IN_VMEM] * (1 + len(came)),
        out_shape=jax.ShapeDtypeStruct((rows, cells), came[0].dtype),
        compiler_params=SMALL,
    )(own, *came)


def couple(kq, lines, twins, others, steps, bands, modes, last, before=None):
    parts = len(others)
    half = parts // 2
    cells = others[0].shape[1]
    wide = parts * cells
    rows = 2 * bands
    share = lines.shape[1] - rows
    pairs = modes // 2

    def kernel(kq_ref, lines_ref, twins_ref, *refs):
        other_refs, refs = refs[:parts], refs[parts:]
        if before is not None:
            before_ref, *refs = refs
        out_ref, wave_re, wave_im, pots, left, right_a, right_b, *more = refs
        result, sems = more if last else (out_ref, None)

        def copy(pair):
            at = pl.ds(2 * pair, 2)
            return pltpu.make_async_copy(result.at[at], out_ref.at[at], sems.at[pair])

        first = lax.axis_index("c") * (share // 2)
        zl = lax.axis_index("zl")
        crossed = kq_ref[0] // 16 != lax.axis_index("zh")
        for p in range(parts):
            at = slice(p * cells, (p + 1) * cells)
            s = steps[p % half]
            turned = lax.rem(2 * zl + 5 - s, 4)
            turned = jnp.where(turned == 2, 3, jnp.where(turned == 3, 2, turned))
            index = jnp.where(crossed, turned, STEPS.index(s))
            source = lines_ref if p < half else twins_ref
            wave_re[:, at] = source[index, :bands].astype(jnp.float32)
            wave_im[:, at] = source[index, bands:rows].astype(jnp.float32)
            pots[:, at] = source[index, rows:].astype(jnp.float32)
            left[:, at] = other_refs[p][...]

        def fill(mode, right):
            for p in range(parts):
                at = slice(p * cells, (p + 1) * cells)
                dv_re = pots[pl.ds(first + 2 * mode, 1), at]
                dv_im = pots[pl.ds(first + 2 * mode + 1, 1), at]
                w_re, w_im = wave_re[:, at], wave_im[:, at]
                right[:bands, at] = (dv_re * w_re - dv_im * w_im).astype(jnp.bfloat16)
                right[bands:, at] = (dv_re * w_im + dv_im * w_re).astype(jnp.bfloat16)

        def finish(mode, right):
            full = lax.dot_general(left[...], right[...], (((1,), (1,)), ((), ())), preferred_element_type=jnp.float32)
            real = full[:bands, :bands] + full[bands:, bands:]
            imag = full[:bands, bands:] - full[bands:, :bands]
            if before is not None:
                real, imag = real + before_ref[mode, 0], imag + before_ref[mode, 1]
            result[mode, 0] = real
            result[mode, 1] = imag

        fill(0, right_a)
        for pair in range(pairs):
            fill(2 * pair + 1, right_b)
            finish(2 * pair, right_a)
            if pair + 1 < pairs:
                fill(2 * pair + 2, right_a)
            finish(2 * pair + 1, right_b)
            if last:
                copy(pair).start()
        if last:
            for pair in range(pairs):
                copy(pair).wait()

    total = (modes, 2, bands, bands)
    scratch = [
        pltpu.VMEM((bands, wide), jnp.float32),
        pltpu.VMEM((bands, wide), jnp.float32),
        pltpu.VMEM((share, wide), jnp.float32),
        pltpu.VMEM((rows, wide), jnp.bfloat16),
        pltpu.VMEM((rows, wide), jnp.bfloat16),
        pltpu.VMEM((rows, wide), jnp.bfloat16),
    ]
    if last:
        scratch += [pltpu.VMEM(total, jnp.float32), pltpu.SemaphoreType.DMA((pairs,))]
    args = [kq, lines, twins, *others]
    specs = [IN_SMEM] + [IN_VMEM] * (2 + parts)
    if before is not None:
        args, specs = args + [before], specs + [IN_VMEM]
    return pl.pallas_call(
        kernel,
        in_specs=specs,
        out_specs=pl.BlockSpec(memory_space=pl.ANY) if last else IN_VMEM,
        out_shape=jax.ShapeDtypeStruct(total, jnp.float32),
        scratch_shapes=scratch,
        compiler_params=SMALL,
    )(*args)


def body(psi, dvscf, kq_map):
    bands, cells = psi.shape[2], psi.shape[3]
    modes = dvscf.shape[0] // 8
    slab = psi.reshape(2 * bands, cells)

    swapped = lax.ppermute(slab, ("zh", "zl"), MIRROR)
    packs = pack_lines(slab, dvscf)
    tag = jnp.broadcast_to(kq_map, (8, 128))
    near = [slab] + [lax.ppermute(slab, "y", ring(STEPS[i])) for i in (1, 2, 3)]
    far = [swapped] + [lax.ppermute(swapped, "y", ring(STEPS[i])) for i in (1, 2, 3)]
    wanted = [tag] + [lax.ppermute(tag, "x", ring(-STEPS[i])) for i in (1, 2, 3)]
    lines = [packs[0]] + [lax.ppermute(packs[i], "zl", ring(STEPS[i])) for i in (1, 2, 3)]
    lines = jnp.stack(lines)
    twins = lax.ppermute(lines, "c", SWAP)
    slots = choose(wanted, near + far)
    came = [slots[0]] + [lax.ppermute(slots[i], "x", ring(STEPS[i])) for i in (1, 2, 3)]
    phi = keep(tag, came)

    others = [phi] + [lax.ppermute(phi, "zl", ring(STEPS[i])) for i in (1, 2, 3)]
    mates = [lax.ppermute(o, "c", SWAP) for o in others]
    out = None
    for name, at in (("early", slice(0, 1)), ("middle", slice(1, 3)), ("late", slice(3, 4))):
        out = couple(kq_map, lines, twins, others[at] + mates[at], STEPS[at], bands, modes, name == "late", out)
    return out[:, None]


def solution(mesh):
    finer = Mesh(mesh.devices.reshape(2, 4, 4, 4, 2), KA + GA)
    in_specs = (P(KA, None, None, GA), P(None, None, GA), P(KA))
    out_specs = P(GA, KA, None, None, None)
    return jax.shard_map(body, mesh=finer, in_specs=in_specs, out_specs=out_specs, check_vma=False)
```

```python
import jax
import jax.numpy as jnp
from jax import lax
from jax.experimental import pallas as pl
from jax.experimental.pallas import tpu as pltpu
from jax.sharding import Mesh
from jax.sharding import PartitionSpec as P

KA = ("zh", "x", "y")
GA = ("zl", "c")
SWAP = [(0, 1), (1, 0)]
MIRROR = [(z, 7 - z) for z in range(8)]
STEPS = (0, 1, 3, 2)
SMALL = pltpu.CompilerParams(vmem_limit_bytes=20 * 2**20)
IN_SMEM = pl.BlockSpec(memory_space=pltpu.SMEM)
IN_VMEM = pl.BlockSpec(memory_space=pltpu.VMEM)


def ring(step, size=4):
    return [(i, (i + step) % size) for i in range(size)]


def pack_lines(slab, potential):
    rows, cells = slab.shape
    modes = potential.shape[0] // 4

    def kernel(slab_ref, pot_ref, *outs):
        zl = lax.axis_index("zl")
        for s, out in zip(STEPS, outs):
            out[:rows] = slab_ref[...]
            first = modes * lax.rem(zl + s, 4)
            for m in range(modes):
                out[rows + 2 * m : rows + 2 * m + 2] = pot_ref[first + m]

    return pl.pallas_call(
        kernel,
        in_specs=[IN_VMEM, IN_VMEM],
        out_shape=[jax.ShapeDtypeStruct((rows + 2 * modes, cells), slab.dtype)] * 4,
        compiler_params=SMALL,
    )(slab, potential)


def number_in(ref):
    return jnp.max(ref[...].astype(jnp.float32)).astype(jnp.int32)


def pick(number, values):
    out = values[0]
    for i, value in enumerate(values[1:], 1):
        out = jnp.where(number == i, value, out)
    return out


def choose(wanted, blocks):
    count = len(wanted)
    rows, cells = blocks[0].shape

    def kernel(*refs):
        numbers = [number_in(ref) for ref in refs[:count]]
        held, outs = refs[count : count + len(blocks)], refs[count + len(blocks) :]
        zh, y = lax.axis_index("zh"), lax.axis_index("y")
        places = []
        for number in numbers:
            back = lax.rem(y + 4 - lax.rem(number, 4), 4)
            back = jnp.where(back == 2, 3, jnp.where(back == 3, 2, back))
            places.append(jnp.where(number // 16 == zh, back, back + 4))
        for at in range(0, rows, 16):
            values = [ref[at : at + 16] for ref in held]
            for place, out in zip(places, outs):
                out[at : at + 16] = pick(place, values)

    return pl.pallas_call(
        kernel,
        in_specs=[IN_VMEM] * (count + len(blocks)),
        out_shape=[jax.ShapeDtypeStruct((rows, cells), blocks[0].dtype)] * count,
        compiler_params=SMALL,
    )(*wanted, *blocks)


def keep(own, came):
    rows, cells = came[0].shape

    def kernel(own_ref, *refs):
        number = number_in(own_ref)
        back = lax.rem(lax.axis_index("x") + 4 - lax.rem(number // 4, 4), 4)
        back = jnp.where(back == 2, 3, jnp.where(back == 3, 2, back))
        for at in range(0, rows, 16):
            refs[-1][at : at + 16] = pick(back, [ref[at : at + 16] for ref in refs[:-1]])

    return pl.pallas_call(
        kernel,
        in_specs=[IN_VMEM] * (1 + len(came)),
        out_shape=jax.ShapeDtypeStruct((rows, cells), came[0].dtype),
        compiler_params=SMALL,
    )(own, *came)


def couple(kq, lines, twins, others, pieces, bands, modes, last, before=None):
    parts = len(others)
    cells = others[0].shape[1]
    wide = parts * cells
    rows = 2 * bands
    share = lines.shape[1] - rows
    pairs = modes // 2

    def kernel(kq_ref, lines_ref, twins_ref, *refs):
        other_refs, refs = refs[:parts], refs[parts:]
        if before is not None:
            before_ref, *refs = refs
        out_ref, wave_re, wave_im, pots, left, right_a, right_b, *more = refs
        result, sems = more if last else (out_ref, None)

        def copy(pair):
            at = pl.ds(2 * pair, 2)
            return pltpu.make_async_copy(result.at[at], out_ref.at[at], sems.at[pair])

        first = lax.axis_index("c") * (share // 2)
        zl = lax.axis_index("zl")
        crossed = kq_ref[0] // 16 != lax.axis_index("zh")
        for p in range(parts):
            at = slice(p * cells, (p + 1) * cells)
            s, twin = pieces[p]
            turned = lax.rem(2 * zl + 5 - s, 4)
            turned = jnp.where(turned == 2, 3, jnp.where(turned == 3, 2, turned))
            index = jnp.where(crossed, turned, STEPS.index(s))
            source = twins_ref if twin else lines_ref
            wave_re[:, at] = source[index, :bands].astype(jnp.float32)
            wave_im[:, at] = source[index, bands:rows].astype(jnp.float32)
            pots[:, at] = source[index, rows:].astype(jnp.float32)
            left[:, at] = other_refs[p][...]

        def fill(mode, right):
            for p in range(parts):
                at = slice(p * cells, (p + 1) * cells)
                dv_re = pots[pl.ds(first + 2 * mode, 1), at]
                dv_im = pots[pl.ds(first + 2 * mode + 1, 1), at]
                w_re, w_im = wave_re[:, at], wave_im[:, at]
                right[:bands, at] = (dv_re * w_re - dv_im * w_im).astype(jnp.bfloat16)
                right[bands:, at] = (dv_re * w_im + dv_im * w_re).astype(jnp.bfloat16)

        def finish(mode, right):
            full = lax.dot_general(left[...], right[...], (((1,), (1,)), ((), ())), preferred_element_type=jnp.float32)
            real = full[:bands, :bands] + full[bands:, bands:]
            imag = full[:bands, bands:] - full[bands:, :bands]
            if before is not None:
                real, imag = real + before_ref[mode, 0], imag + before_ref[mode, 1]
            result[mode, 0] = real
            result[mode, 1] = imag

        fill(0, right_a)
        for pair in range(pairs):
            fill(2 * pair + 1, right_b)
            finish(2 * pair, right_a)
            if pair + 1 < pairs:
                fill(2 * pair + 2, right_a)
            finish(2 * pair + 1, right_b)
            if last:
                copy(pair).start()
        if last:
            for pair in range(pairs):
                copy(pair).wait()

    total = (modes, 2, bands, bands)
    scratch = [
        pltpu.VMEM((bands, wide), jnp.float32),
        pltpu.VMEM((bands, wide), jnp.float32),
        pltpu.VMEM((share, wide), jnp.float32),
        pltpu.VMEM((rows, wide), jnp.bfloat16),
        pltpu.VMEM((rows, wide), jnp.bfloat16),
        pltpu.VMEM((rows, wide), jnp.bfloat16),
    ]
    if last:
        scratch += [pltpu.VMEM(total, jnp.float32), pltpu.SemaphoreType.DMA((pairs,))]
    args = [kq, lines, twins, *others]
    specs = [IN_SMEM] + [IN_VMEM] * (2 + parts)
    if before is not None:
        args, specs = args + [before], specs + [IN_VMEM]
    return pl.pallas_call(
        kernel,
        in_specs=specs,
        out_specs=pl.BlockSpec(memory_space=pl.ANY) if last else IN_VMEM,
        out_shape=jax.ShapeDtypeStruct(total, jnp.float32),
        scratch_shapes=scratch,
        compiler_params=SMALL,
    )(*args)


def body(psi, dvscf, kq_map):
    bands, cells = psi.shape[2], psi.shape[3]
    modes = dvscf.shape[0] // 8
    slab = psi.reshape(2 * bands, cells)

    swapped = lax.ppermute(slab, ("zh", "zl"), MIRROR)
    packs = pack_lines(slab, dvscf)
    tag = jnp.broadcast_to(kq_map, (8, 128))
    near = [slab] + [lax.ppermute(slab, "y", ring(STEPS[i])) for i in (1, 2, 3)]
    far = [swapped] + [lax.ppermute(swapped, "y", ring(STEPS[i])) for i in (1, 2, 3)]
    wanted = [tag] + [lax.ppermute(tag, "x", ring(-STEPS[i])) for i in (1, 2, 3)]
    lines = [packs[0]] + [lax.ppermute(packs[i], "zl", ring(STEPS[i])) for i in (1, 2, 3)]
    slots = choose(wanted, near + far)
    came = [slots[0]] + [lax.ppermute(slots[i], "x", ring(STEPS[i])) for i in (1, 2, 3)]
    phi = keep(tag, came)
    lines = jnp.stack(lines)
    twins = lax.ppermute(lines, "c", SWAP)

    others = [phi] + [lax.ppermute(phi, "zl", ring(STEPS[i])) for i in (1, 2, 3)]
    mates = [lax.ppermute(o, "c", SWAP) for o in others]
    out = None
    for name, values, pieces in (
        ("early", (others[0], mates[0]), ((0, False), (0, True))),
        ("middle", others[1:3], ((1, False), (3, False))),
        ("paired", mates[1:3], ((1, True), (3, True))),
        ("final", others[3:], ((2, False),)),
        ("last", mates[3:], ((2, True),)),
    ):
        out = couple(kq_map, lines, twins, values, pieces, bands, modes, name == "last", out)
    return out[:, None]


def solution(mesh):
    finer = Mesh(mesh.devices.reshape(2, 4, 4, 4, 2), KA + GA)
    in_specs = (P(KA, None, None, GA), P(None, None, GA), P(KA))
    out_specs = P(GA, KA, None, None, None)
    return jax.shard_map(body, mesh=finer, in_specs=in_specs, out_specs=out_specs, check_vma=False)
```
